32 devices in a mesh: tm: 16 (over z, x, core), tile: 2 (over y).
Axes of the slice: x: 2, y: 2, z: 4, core: 2. Of those that a mesh axis runs over, the one named last changes fastest.
Arguments:
- queries: bfloat16 [32, 4, 64, 2560], P('tm', 'tile'), may hold values from -40 to 40
- keys: bfloat16 [32, 4, 64, 2560], P('tm', 'tile'), may hold values from -6 to 6
- values: bfloat16 [32, 4, 64, 2560], P('tm', 'tile'), may hold values from -6 to 6
- neighbours: int32 [16, 2, 3], P('tm', 'tile'), may hold values from -1 to 14, as said below
- halo_rows: int32 [16, 2], P('tm', 'tile'), may hold values from 0 to 2, as said below
Outputs:
- attended: bfloat16 [32, 4, 64, 2560], P('tm', 'tile')
The draws below stay inside these ranges and needn't reach their ends.
Inputs may be any that keep to these rules, and one draw needn't show every extreme that they name: `neighbours`: for frame block b and tile t, the entries that are not -1 are distinct frame blocks from max(0, b - 5) to b - 1; lists hold 0 to 3 entries, and some list is full. `halo_rows`: some frame block and tile reads 2 rows.
All inputs are finite; a program needn't handle non-finite values.
Results may differ from the reference program's by a relative error of at most 0.0046.
Values may be sent and summed in bfloat16 or wider, within the bound.
No kernel may reach another device: no remote copies, remote signals or barrier semaphores. Data moves between devices by JAX's collectives and lax.ppermute only.
A program may use at most 128 MiB of HBM per device.

```python
import math
import jax
import jax.numpy as jnp
from jax import lax

HEADS = 20
HD = 128
GRID_W = 64
FR_DEV = 2
TROWS = 2
HMAX = 2
NB = 3
WIN = 5
CHANNELS = 2560
BLOCKS = 16
TILES = 2
FRAMES = 32
GRID_H = 4


def drawn_pair(key):
    base = jax.random.fold_in(key, 11)
    query_seed, keys_seed = jax.random.split(base, 2)
    shape = (FRAMES, GRID_H, GRID_W, HEADS, HD)
    query_base = jnp.clip(jax.random.normal(query_seed, shape, jnp.float32), -6.0, 6.0)
    key_base = jnp.clip(jax.random.normal(keys_seed, shape, jnp.float32), -6.0, 6.0)
    flat_shape = (FRAMES, GRID_H, GRID_W, HEADS * HD)
    return (query_base.reshape(flat_shape), key_base.reshape(flat_shape))


def draw_queries(key, part):
    return drawn_pair(key)[0].astype(jnp.bfloat16)


def draw_keys(key, part):
    return drawn_pair(key)[1].astype(jnp.bfloat16)


def draw_neighbours(key, part):
    base = jax.random.fold_in(key, 31)
    bits_seed, length_seed = jax.random.split(base)
    random_bits = jax.random.randint(bits_seed, (BLOCKS, TILES, WIN), 0, 1 << 20)
    offsets = jnp.arange(1, WIN + 1, dtype=jnp.int32)
    block_pos = jnp.arange(BLOCKS, dtype=jnp.int32)[:, None, None]
    usable = block_pos - offsets[None, None, :] >= 0
    ranked = jnp.where(usable, random_bits * WIN + offsets - 1 + WIN, offsets - 1 + jnp.zeros_like(random_bits))
    top_vals, top_idx = lax.top_k(ranked, NB)
    chosen = top_idx.astype(jnp.int32) + 1
    list_length = jax.random.randint(length_seed, (BLOCKS, TILES), 0, NB + 1)
    list_length = list_length.at[BLOCKS - 1, 0].set(NB)
    slot_index = jnp.arange(NB, dtype=jnp.int32)[None, None, :]
    block_ids = block_pos - chosen
    kept_mask = (slot_index < list_length[:, :, None]) & (block_ids >= 0)
    return jnp.where(kept_mask, block_ids, -1).astype(jnp.int32)


def draw_halo_rows(key, part):
    widths = jax.random.randint(jax.random.fold_in(key, 23), (BLOCKS, TILES), 0, HMAX + 1)
    return widths.at[BLOCKS - 1, 0].set(HMAX).astype(jnp.int32)


def levels(key, shape, pieces, low, high):
    level, own = 1.0, jax.random.fold_in(key, 6)
    for axis_at, shards_of in pieces:
        draws = jnp.exp(jax.random.uniform(jax.random.fold_in(own, axis_at), (shards_of,), jnp.float32, low / len(pieces), high / len(pieces)))
        level = level * jnp.repeat(draws, shape[axis_at] // shards_of).reshape([-1 if axis == axis_at else 1 for axis in range(len(shape))])
    return level


def normal_values(key, shape, spread, bound, cuts=(), kind=jnp.bfloat16):
    factor_of = levels(key, shape, cuts, -0.22, 0.18) if cuts else 1.0
    array = jax.random.normal(key, shape, jnp.float32) * spread * factor_of
    return jnp.minimum(jnp.maximum(array, -bound), bound).astype(kind)


def setup_inputs(seed: int = 0) -> dict:
    key_list = jax.random.split(jax.random.key(seed), 6)
    return {
        "queries": draw_queries(jax.random.fold_in(key_list[5], 71), 0),
        "keys": draw_keys(jax.random.fold_in(key_list[5], 71), 0),
        "values": normal_values(key_list[2], (FRAMES, GRID_H, GRID_W, CHANNELS), 1.0, 6.0, ((0, 16), (1, 2))),
        "neighbours": draw_neighbours(jax.random.fold_in(key_list[5], 71), 0),
        "halo_rows": draw_halo_rows(jax.random.fold_in(key_list[5], 71), 0),
    }


def attend(query_rows, key_rows, value_rows, allowed):
    tokens, channels = query_rows.shape
    head_count = channels // HD
    key_count = key_rows.shape[0]
    query_heads = query_rows.astype(jnp.float32).reshape(tokens, head_count, HD)
    key_heads = key_rows.astype(jnp.float32).reshape(key_count, head_count, HD)
    value_heads = value_rows.astype(jnp.float32).reshape(key_count, head_count, HD)
    scores = jnp.einsum('qhd,khd->hqk', query_heads, key_heads) / math.sqrt(HD)
    scores = jnp.where(allowed[None], scores, -jnp.inf)
    maximum = lax.optimization_barrier(jnp.max(scores, axis=2, keepdims=True))
    weights = jnp.where(allowed[None], jnp.exp(scores - maximum), 0.0)
    totals = lax.optimization_barrier(jnp.sum(weights, axis=2))
    rounded = lax.optimization_barrier(weights.astype(jnp.bfloat16)).astype(jnp.float32)
    numerator = jnp.einsum('hqk,khd->qhd', rounded, value_heads)
    return (numerator / totals.T[:, :, None]).reshape(tokens, channels).astype(jnp.bfloat16)

def reference(queries, keys, values, neighbours, halo_rows):
    channels = queries.shape[3]
    tokens = FR_DEV * TROWS * GRID_W
    span_rows = TROWS + 2 * HMAX
    pad_keys = jnp.pad(keys, ((0, 0), (HMAX, HMAX), (0, 0), (0, 0)))
    pad_values = jnp.pad(values, ((0, 0), (HMAX, HMAX), (0, 0), (0, 0)))
    anchor = jnp.zeros((), jnp.int32)
    query_frame = lax.broadcasted_iota(jnp.int32, (FR_DEV, TROWS, GRID_W), 0).reshape(-1)
    key_frame = lax.broadcasted_iota(jnp.int32, (FR_DEV, span_rows, GRID_W), 0).reshape(-1)
    key_row = lax.broadcasted_iota(jnp.int32, (FR_DEV, span_rows, GRID_W), 1).reshape(-1)

    def one_device(device):
        block_index = (device // TILES).astype(jnp.int32)
        tile_index = (device % TILES).astype(jnp.int32)
        frame_start = (block_index * FR_DEV).astype(jnp.int32)
        row_start = (tile_index * TROWS).astype(jnp.int32)
        query_rows = lax.dynamic_slice(queries, (frame_start, row_start, anchor, anchor), (FR_DEV, TROWS, GRID_W, channels)).reshape(tokens, channels)
        own_keys = lax.dynamic_slice(pad_keys, (frame_start, row_start, anchor, anchor), (FR_DEV, span_rows, GRID_W, channels)).reshape(-1, channels)
        own_values = lax.dynamic_slice(pad_values, (frame_start, row_start, anchor, anchor), (FR_DEV, span_rows, GRID_W, channels)).reshape(-1, channels)
        listed = neighbours[block_index, tile_index]
        halo_reach = halo_rows[block_index, tile_index]

        def fetch_rows(block_id):
            start_frame = (jnp.maximum(block_id, 0) * FR_DEV).astype(jnp.int32)
            far_keys = lax.dynamic_slice(keys, (start_frame, row_start, anchor, anchor), (FR_DEV, TROWS, GRID_W, channels))
            far_values = lax.dynamic_slice(values, (start_frame, row_start, anchor, anchor), (FR_DEV, TROWS, GRID_W, channels))
            return (far_keys, far_values)
        far_keys, far_values = jax.vmap(fetch_rows)(listed)
        global_row = row_start - HMAX + key_row
        row_ok = (global_row >= 0) & (global_row < GRID_H) & (key_row >= HMAX - halo_reach) & (key_row < HMAX + TROWS + halo_reach)
        own_mask = (key_frame[None, :] <= query_frame[:, None]) & row_ok[None, :]
        slot_mask = jnp.repeat(listed >= 0, tokens)
        allowed = jnp.concatenate((own_mask, jnp.broadcast_to(slot_mask[None, :], (tokens, slot_mask.shape[0]))), axis=1)
        key_rows = jnp.concatenate((own_keys, far_keys.reshape(-1, channels)), axis=0)
        value_rows = jnp.concatenate((own_values, far_values.reshape(-1, channels)), axis=0)
        return attend(query_rows, key_rows, value_rows, allowed)
    results = lax.map(one_device, jnp.arange(BLOCKS * TILES, dtype=jnp.int32))
    results = results.reshape(BLOCKS, TILES, FR_DEV, TROWS, GRID_W, channels)
    return results.transpose(0, 2, 1, 3, 4, 5).reshape(FRAMES, GRID_H, GRID_W, channels)
```

```python
import functools
import math

import jax
import jax.numpy as jnp
from jax import lax
from jax.experimental import pallas as pl
from jax.experimental.pallas import tpu as pltpu
from jax.sharding import PartitionSpec as P

HD = 128
HMAX = 2
LEVEL = 4
CHUNKS = (8, 7, 5)
NEG = -1e30
SCALE = math.log2(math.e) / math.sqrt(HD)


def scores_of(query, key):
    return lax.dot_general(query, key, (((1,), (1,)), ((), ())), preferred_element_type=jnp.float32)


def wide(column, like):
    return jnp.broadcast_to(column[:, :1], like.shape)


def weigh(scores, maximum, value):
    weights = jnp.exp2((scores - wide(maximum, scores)) * SCALE).astype(jnp.bfloat16)
    ones = jnp.ones((value.shape[0], HD), jnp.bfloat16)
    return lax.dot_general(
        weights,
        jnp.concatenate([value, ones], axis=1),
        (((1,), (0,)), ((), ())),
        preferred_element_type=jnp.float32,
    )


def add_block(rows, query, key, value, mask, max_ref, sum_ref):
    scores = scores_of(query, key)
    if mask is not None:
        scores = jnp.where(mask, scores, NEG)
    before = max_ref[rows, :]
    after = jnp.maximum(before, jnp.max(scores, axis=1, keepdims=True))
    kept = jnp.exp2((before - after) * SCALE)
    max_ref[rows, :] = after
    sum_ref[rows, :] = sum_ref[rows, :] * jnp.concatenate([kept, kept], axis=1) + weigh(
        scores, after, value
    )


def later_kernel(heads, flags, q_ref, k_ref, v_ref, *refs):
    others, (ret_ref, max_ref, sum_ref, stat_ref) = refs[:-4], refs[-4:]
    head = pl.program_id(0)
    tokens = q_ref.shape[0]
    rows = pl.ds(0, tokens)
    max_ref[...] = jnp.full(max_ref.shape, NEG, jnp.float32)
    sum_ref[...] = jnp.zeros(sum_ref.shape, jnp.float32)
    query = q_ref[...]

    @pl.when(head == 0)
    def _():
        stat_ref[...] = jnp.zeros(stat_ref.shape, jnp.float32)

    @pl.when(flags[0] > 0)
    def _():
        add_block(rows, query, k_ref[...], v_ref[...], None, max_ref, sum_ref)

    for at, other in enumerate(others):

        @pl.when(flags[1 + at] > 0)
        def _(other=other):
            add_block(rows, query, other[0], other[1], None, max_ref, sum_ref)

    maximum = max_ref[...]
    sent = maximum.astype(jnp.bfloat16).astype(jnp.float32)
    factor = jnp.exp2((maximum - sent) * SCALE)
    ret_ref[:, pl.ds(pl.multiple_of(head * HD, HD), HD)] = (sum_ref[:, :HD] * factor).astype(
        jnp.bfloat16
    )
    total = sum_ref[:, HD:] * factor
    high = total.astype(jnp.bfloat16).astype(jnp.float32)
    lane = lax.broadcasted_iota(jnp.int32, stat_ref.shape, 1) - 3 * head
    stat = stat_ref[...]
    stat = jnp.where(lane == 0, sent, stat)
    stat = jnp.where(lane == 1, high, stat)
    stat = jnp.where(lane == 2, total - high, stat)
    stat_ref[...] = stat

    @pl.when(head == heads - 1)
    def _():
        ret_ref[:, heads * HD :] = stat_ref[...].astype(jnp.bfloat16)


def own_kernel(shape, halo_count, flags, q_ref, k_ref, v_ref, *refs):
    frames, tile_rows, grid_columns = shape
    per_frame = tile_rows * grid_columns
    halos = refs[:halo_count]
    others = refs[halo_count : halo_count + 3]
    num_ref, stat_ref = refs[halo_count + 3 : halo_count + 5]
    out_ref, max_ref, sum_ref = refs[-3:]
    head = pl.program_id(0)
    tokens = frames * per_frame
    for frame in range(frames):
        rows = pl.ds(frame * per_frame, per_frame)
        seen = (frame + 1) * per_frame
        scores = scores_of(q_ref[rows, :], k_ref[:seen, :])
        maximum = jnp.max(scores, axis=1, keepdims=True)
        max_ref[rows, :] = jnp.broadcast_to(maximum, (per_frame, HD))
        sum_ref[rows, :] = weigh(scores, maximum, v_ref[:seen, :])
    for at, halo in enumerate(halos):
        low, high = flags[4 + 2 * at], flags[5 + 2 * at]

        @pl.when(high > low)
        def _(halo=halo, low=low, high=high):
            for frame in range(frames):
                rows = pl.ds(frame * per_frame, per_frame)
                seen = (frame + 1) * per_frame
                position = lax.broadcasted_iota(jnp.int32, (per_frame, seen), 1)
                mask = None
                for past in range(frame + 1):
                    place = position - past * per_frame
                    inside = (place >= low * grid_columns) & (place < high * grid_columns)
                    mask = inside if mask is None else mask | inside
                add_block(
                    rows, q_ref[rows, :], halo[0, :seen], halo[1, :seen], mask, max_ref, sum_ref
                )

    for at, other in enumerate(others):

        @pl.when(flags[at] > 0)
        def _(other=other):
            add_block(
                pl.ds(0, tokens), q_ref[...], other[0], other[1], None, max_ref, sum_ref
            )

    @pl.when(flags[3] == 0)
    def _():
        out_ref[...] = (sum_ref[:, :HD] / sum_ref[:, HD:]).astype(jnp.bfloat16)

    @pl.when(flags[3] > 0)
    def _():
        lane = lax.broadcasted_iota(jnp.int32, (tokens, HD), 1) - 3 * head
        stat = stat_ref[...].astype(jnp.float32)

        def pick(select):
            return jnp.sum(jnp.where(select, stat, 0.0), axis=1, keepdims=True)

        theirs = pick(lane == 0)
        their_total = pick((lane == 1) | (lane == 2))
        mine = max_ref[...]
        both = jnp.maximum(mine, theirs)
        keep = jnp.exp2((mine - both) * SCALE)
        take = jnp.exp2((theirs - both) * SCALE)
        numerator = sum_ref[:, :HD] * keep + num_ref[...].astype(jnp.float32) * take
        total = sum_ref[:, HD:] * keep + their_total * take
        out_ref[...] = (numerator / total).astype(jnp.bfloat16)


def estimate(tokens, keys, heads):
    return pl.CostEstimate(
        flops=4 * tokens * keys * heads * HD,
        bytes_accessed=8 * tokens * heads * HD,
        transcendentals=tokens * keys * heads,
    )


def head_spec(tokens, first):
    return pl.BlockSpec((tokens, HD), lambda h, f: (0, first + h))


def pair_spec(tokens, first):
    return pl.BlockSpec((2, tokens, HD), lambda h, f: (0, 0, first + h))


def later_sums(flags, query, keys, values, first, heads, others):
    tokens = query.shape[0]
    return pl.pallas_call(
        functools.partial(later_kernel, heads),
        grid_spec=pltpu.PrefetchScalarGridSpec(
            num_scalar_prefetch=1,
            grid=(heads,),
            in_specs=[head_spec(tokens, first)] * 3
            + [pair_spec(tokens, start) for _, start in others],
            out_specs=pl.BlockSpec((tokens, (heads + 1) * HD), lambda h, f: (0, 0)),
            scratch_shapes=[
                pltpu.VMEM((tokens, HD), jnp.float32),
                pltpu.VMEM((tokens, 2 * HD), jnp.float32),
                pltpu.VMEM((tokens, HD), jnp.float32),
            ],
        ),
        out_shape=jax.ShapeDtypeStruct((tokens, (heads + 1) * HD), jnp.bfloat16),
        cost_estimate=estimate(tokens, 3 * tokens, heads),
        name="later",
    )(flags, query, keys, values, *[pair for pair, _ in others])


def own_attention(flags, query, keys, values, first, heads, halos, others, returned, out, shape):
    tokens, channels = query.shape
    operands = [query, keys, values]
    specs = [head_spec(tokens, first)] * 3
    for pair, start in halos + others:
        operands.append(pair)
        specs.append(pair_spec(tokens, start))
    operands += [returned, returned]
    specs += [
        head_spec(tokens, 0),
        pl.BlockSpec((tokens, HD), lambda h, f: (0, heads)),
    ]
    aliases = {}
    if out is not None:
        operands.append(out)
        specs.append(pl.BlockSpec(memory_space=pl.ANY))
        aliases = {len(operands): 0}
    return pl.pallas_call(
        functools.partial(own_kernel, shape, len(halos)),
        grid_spec=pltpu.PrefetchScalarGridSpec(
            num_scalar_prefetch=1,
            grid=(heads,),
            in_specs=specs,
            out_specs=head_spec(tokens, first),
            scratch_shapes=[
                pltpu.VMEM((tokens, HD), jnp.float32),
                pltpu.VMEM((tokens, 2 * HD), jnp.float32),
            ],
        ),
        out_shape=jax.ShapeDtypeStruct((tokens, channels), jnp.bfloat16),
        input_output_aliases=aliases,
        cost_estimate=estimate(tokens, 5 * tokens, heads),
        name="own",
    )(flags, *operands)


def local(queries, keys, values, neighbours, halo_rows):
    frames, tile_rows, grid_columns, channels = queries.shape
    tokens = frames * tile_rows * grid_columns
    blocks, tiles = lax.axis_size("tm"), lax.axis_size("tile")
    block, tile = lax.axis_index("tm"), lax.axis_index("tile")
    assert blocks % LEVEL == 0 and HMAX <= tile_rows

    def shifted(value, axis, steps):
        size = lax.axis_size(axis)
        return lax.ppermute(
            value, axis, [(i, i + steps) for i in range(size) if 0 <= i + steps < size]
        )

    def swapped(value, bit):
        return lax.ppermute(value, "tm", [(i, i ^ bit) for i in range(blocks)])

    query = queries.reshape(tokens, channels)
    key = keys.reshape(tokens, channels)
    value = values.reshape(tokens, channels)
    bounds, first = [], 0
    for heads in CHUNKS:
        bounds.append((first, heads))
        first += heads
    assert first * HD == channels

    pairs = [
        jnp.stack((key[:, a * HD : (a + n) * HD], value[:, a * HD : (a + n) * HD]))
        for a, n in bounds
    ]
    across, halos = [], []
    for pair in pairs:
        across.append(swapped(pair, 2))
        if tiles == 2:
            halos.append([lax.ppermute(pair, "tile", [(0, 1), (1, 0)])])
        else:
            halos.append([shifted(pair, "tile", 1), shifted(pair, "tile", -1)])
    next_query = shifted(query, "tm", -LEVEL)
    next_listed = shifted(neighbours[0, 0], "tm", -LEVEL)
    beside = [swapped(pair, 1) for pair in pairs]
    corner = [swapped(pair, 1) for pair in across]
    below = [
        lax.ppermute(
            pair,
            "tm",
            [(i, i + LEVEL - 1) for i in range(1, blocks - LEVEL + 1, LEVEL)],
        )
        for pair in across
    ]

    listed = neighbours[0, 0]
    reach = halo_rows[0, 0]
    level_start = block - block % LEVEL

    def holds(array, number):
        return jnp.any(array == number).astype(jnp.int32)

    has_next = (block + LEVEL < blocks).astype(jnp.int32)
    later_flags = jnp.stack(
        [has_next * holds(next_listed, block ^ r) for r in range(LEVEL)]
        + [has_next * holds(next_listed, block - 1) * ((block > 0) & (block == level_start))]
    ).astype(jnp.int32)
    above = [tile_rows - reach, jnp.full_like(reach, tile_rows)]
    under = [jnp.zeros_like(reach), reach]
    if tiles == 2:
        spans = [jnp.where(tile == 1, a, u) for a, u in zip(above, under)]
    else:
        spans = [jnp.where(tile > 0, a, 0) for a in above]
        spans += [jnp.where(tile < tiles - 1, u, 0) for u in under]
    own_flags = jnp.stack(
        [holds(listed, block ^ r) for r in range(1, LEVEL)]
        + [jnp.any((listed >= 0) & (listed < level_start)).astype(jnp.int32)]
        + spans
    ).astype(jnp.int32)

    returned = []
    for at, (first, heads) in enumerate(bounds):
        partial_sums = later_sums(
            later_flags,
            next_query,
            key,
            value,
            first,
            heads,
            [(beside[at], 0), (across[at], 0), (corner[at], 0), (below[at], 0)],
        )
        returned.append(shifted(partial_sums, "tm", LEVEL))
    out = None
    for at, (first, heads) in enumerate(bounds):
        out = own_attention(
            own_flags,
            query,
            key,
            value,
            first,
            heads,
            [(halo, 0) for halo in halos[at]],
            [(beside[at], 0), (across[at], 0), (corner[at], 0)],
            returned[at],
            out,
            (frames, tile_rows, grid_columns),
        )
    return out.reshape(frames, tile_rows, grid_columns, channels)


def solution(mesh):
    return jax.shard_map(
        local,
        mesh=mesh,
        in_specs=(
            P("tm", "tile", None, None),
            P("tm", "tile", None, None),
            P("tm", "tile", None, None),
            P("tm", "tile", None),
            P("tm", "tile"),
        ),
        out_specs=P("tm", "tile", None, None),
        check_vma=False,
    )
```

```python
import functools
import math

import jax
import jax.numpy as jnp
from jax import lax
from jax.experimental import pallas as pl
from jax.experimental.pallas import tpu as pltpu
from jax.sharding import PartitionSpec as P


HD = 128
HMAX = 2
LEVEL = 4
CHUNKS = (5, 6, 5, 4)
DIRECT = (3,)
EARLY = (0, 1, 2, 3)
NEG = -(2.0**99)
SCALE = math.log2(math.e) / math.sqrt(HD)
VMEM_LIMIT = 24 * 1024 * 1024


def scores_of(key, query):
    return lax.dot_general(key, query, (((1,), (1,)), ((), ())), preferred_element_type=jnp.float32)


def highest(scores):
    return jnp.max(scores, axis=0, keepdims=True)


def weights_of(scores, maximum):
    return jnp.exp2((scores - maximum) * SCALE)


def weighed(value, weights):
    return lax.dot_general(
        value,
        weights.astype(jnp.bfloat16),
        (((0,), (0,)), ((), ())),
        preferred_element_type=jnp.float32,
    )


def total_of(weights):
    return jnp.sum(weights, axis=0, keepdims=True)


def holds(listed, number):
    return functools.reduce(jnp.logical_or, [listed[i] == number for i in range(listed.shape[0])])


def reaches_below(listed, level_start):
    return functools.reduce(
        jnp.logical_or,
        [(listed[i] >= 0) & (listed[i] < level_start) for i in range(listed.shape[0])],
    )


def returned_stats(ret_ref, heads, head, came_back):
    stats = ret_ref[heads * HD :, :].astype(jnp.float32)[3 * head : 3 * head + 3]
    return jnp.where(came_back, stats[0:1], NEG), stats[1:2] + stats[2:3]


def lanes_of(head):
    return slice(head * HD, (head + 1) * HD)


def stat_rows(heads):
    return -(-3 * heads // 16) * 16


def later_kernel(query_first, first, heads, listed, q_ref, k_ref, v_ref, *refs):
    others, (ret_ref, held_ref) = refs[:-2], refs[-2:]
    block, blocks = lax.axis_index("tm"), lax.axis_size("tm")
    slots = held_ref.shape[0]
    has_next = block + LEVEL < blocks
    seen = [has_next & holds(listed, block ^ r) for r in range(LEVEL)]
    seen.append(has_next & (block > 0) & (block % LEVEL == 0) & holds(listed, block - 1))
    own_lanes = slice(first * HD, (first + heads) * HD)

    def put(slot, other):
        if other is None:
            held_ref[slot, 0] = k_ref[:, own_lanes]
            held_ref[slot, 1] = v_ref[:, own_lanes]
        else:
            held_ref[slot] = other[...]

    count = jnp.int32(0)
    for ok, other in zip(seen, [None, *others]):

        @pl.when(ok)
        def _(other=other, slot=jnp.minimum(count, slots - 1)):
            put(slot, other)

        count += ok.astype(jnp.int32)
    for slot in range(slots):

        @pl.when(count <= slot)
        def _(slot=slot):
            put(slot, None)

    filled = [count > slot for slot in range(slots)]

    def scored(head):
        query = q_ref[:, lanes_of(query_first + head)]
        scores = [scores_of(held_ref[i, 0, :, lanes_of(head)], query) for i in range(slots)]
        maximum = functools.reduce(
            jnp.maximum, [jnp.where(ok, highest(s), NEG) for ok, s in zip(filled, scores)]
        )
        return scores, maximum.astype(jnp.bfloat16).astype(jnp.float32)

    stats = []
    ahead = scored(0)
    for head in range(heads):
        scores, sent = ahead
        if head + 1 < heads:
            ahead = scored(head + 1)
        values = [held_ref[i, 1, :, lanes_of(head)] for i in range(slots)]
        weights = [weights_of(s, jnp.where(ok, sent, -NEG)) for ok, s in zip(filled, scores)]
        total = sum(total_of(w) for w in weights)
        numerator = sum(weighed(v, w) for v, w in zip(values, weights))
        high = total.astype(jnp.bfloat16).astype(jnp.float32)
        ret_ref[head * HD : (head + 1) * HD, :] = numerator.astype(jnp.bfloat16)
        stats += [sent, high, total - high]
    spare = stat_rows(heads) - len(stats)
    if spare:
        stats.append(jnp.zeros((spare, stats[0].shape[1]), jnp.float32))
    ret_ref[heads * HD :, :] = jnp.concatenate(stats, axis=0).astype(jnp.bfloat16)


def own_kernel(first, heads, shape, halo_count, early, listed, reach, q_ref, k_ref, v_ref, *refs):
    frames, tile_rows, grid_columns = shape
    per_frame = tile_rows * grid_columns
    halos, others = refs[:halo_count], refs[halo_count : halo_count + LEVEL - 1]
    if early:
        num_ref, stat_ref = refs[-2:]
    else:
        ret_ref = refs[halo_count + LEVEL - 1]
        out_ref, held_ref, sems = refs[-3:]
    block = lax.axis_index("tm")
    tile, tiles = lax.axis_index("tile"), lax.axis_size("tile")
    level_start = block - block % LEVEL
    seen = [holds(listed, block ^ r) for r in range(1, LEVEL)]
    came_back = reaches_below(listed, level_start)
    from_above = [(tile > 0) & (row >= tile_rows - reach[0]) for row in range(tile_rows)]
    from_below = [(tile < tiles - 1) & (row < reach[0]) for row in range(tile_rows)]
    if halo_count == 1:
        spans = [[above | below for above, below in zip(from_above, from_below)]]
    else:
        spans = [from_above, from_below]

    def scored(head, some):
        lanes, part_lanes = lanes_of(first + head), lanes_of(head)
        own_scores, halo_scores, tops = [], [], []
        for frame in range(frames):
            query = q_ref[frame * per_frame : (frame + 1) * per_frame, lanes]
            upto = (frame + 1) * per_frame
            scores = scores_of(k_ref[:upto, lanes], query)
            top = highest(scores)
            own_scores.append(scores)
            halo_scores.append([])
            for halo, span in zip(halos, spans):
                scores = scores_of(halo[0, :upto, part_lanes], query)
                rows = []
                for row in range((frame + 1) * tile_rows):
                    part = scores[row * grid_columns : (row + 1) * grid_columns]
                    ok = span[row % tile_rows]
                    rows.append((part, ok))
                    top = jnp.maximum(top, jnp.where(ok, highest(part), NEG))
                halo_scores[frame].append(rows)
            tops.append(top)
        maximum = jnp.concatenate(tops, axis=1)
        scores = []
        for ok, other in some:
            scores.append(scores_of(other[0, :, part_lanes], q_ref[:, lanes]))
            maximum = jnp.maximum(maximum, jnp.where(ok, highest(scores[-1]), NEG))
        if early:
            return own_scores, halo_scores, scores, None, None, maximum
        theirs, total = returned_stats(ret_ref, heads, head, came_back)
        return own_scores, halo_scores, scores, theirs, total, jnp.maximum(maximum, theirs)

    def finish(head, some, ahead):
        lanes, part_lanes = lanes_of(first + head), lanes_of(head)
        own_scores, halo_scores, scores, theirs, total, maximum = ahead
        if early:
            total, numerator = 0.0, 0.0
        else:
            take = jnp.exp2((theirs - maximum) * SCALE)
            total = total * take
            numerator = ret_ref[head * HD : (head + 1) * HD, :].astype(jnp.float32) * take
        frame_totals, frame_numerators = [], []
        for frame in range(frames):
            upto = (frame + 1) * per_frame
            limit = maximum[:, frame * per_frame : upto]
            weights = weights_of(own_scores[frame], limit)
            part_total = total_of(weights)
            part = weighed(v_ref[:upto, lanes], weights)
            for halo, rows in zip(halos, halo_scores[frame]):
                weights = jnp.concatenate(
                    [weights_of(s, jnp.where(ok, limit, -NEG)) for s, ok in rows], axis=0
                )
                part_total += total_of(weights)
                part += weighed(halo[1, :upto, part_lanes], weights)
            frame_totals.append(part_total)
            frame_numerators.append(part)
        total += jnp.concatenate(frame_totals, axis=1)
        numerator += jnp.concatenate(frame_numerators, axis=1)
        for s, (ok, other) in zip(scores, some):
            weights = weights_of(s, jnp.where(ok, maximum, -NEG))
            total += total_of(weights)
            numerator += weighed(other[1, :, part_lanes], weights)
        if early:
            num_ref[head * HD : (head + 1) * HD, :] = numerator
            stat_ref[2 * head : 2 * head + 1, :] = maximum
            stat_ref[2 * head + 1 : 2 * head + 2, :] = total
        else:
            held_ref[head] = (numerator / total).astype(jnp.bfloat16).T
            copy_of(head).start()

    def copy_of(head):
        return pltpu.make_async_copy(
            held_ref.at[head], out_ref.at[:, lanes_of(first + head)], sems.at[head]
        )

    def attend(some):
        ahead = scored(0, some)
        for head in range(heads):
            now = ahead
            if head + 1 < heads:
                ahead = scored(head + 1, some)
            finish(head, some, now)

    listed_blocks = list(zip(seen, others))
    far = seen[1] | seen[2]

    @pl.when(far)
    def _():
        attend(listed_blocks)

    @pl.when(jnp.logical_not(far))
    def _():
        attend(listed_blocks[:1])

    if not early:
        for head in range(heads):
            copy_of(head).wait()


def merge_kernel(first, heads, listed, num_ref, stat_ref, ret_ref, *refs):
    out_ref, held_ref, sems = refs[-3:]
    block = lax.axis_index("tm")
    came_back = reaches_below(listed, block - block % LEVEL)
    copies = []
    for head in range(heads):
        theirs, their_total = returned_stats(ret_ref, heads, head, came_back)
        mine, my_total = stat_ref[2 * head : 2 * head + 1], stat_ref[2 * head + 1 : 2 * head + 2]
        maximum = jnp.maximum(mine, theirs)
        keep = jnp.exp2((mine - maximum) * SCALE)
        take = jnp.exp2((theirs - maximum) * SCALE)
        rows = slice(head * HD, (head + 1) * HD)
        numerator = num_ref[rows, :] * keep + ret_ref[rows, :].astype(jnp.float32) * take
        total = my_total * keep + their_total * take
        held_ref[head] = (numerator / total).astype(jnp.bfloat16).T
        copies.append(
            pltpu.make_async_copy(
                held_ref.at[head], out_ref.at[:, lanes_of(first + head)], sems.at[head]
            )
        )
        copies[-1].start()
    for copy in copies:
        copy.wait()


def estimate(tokens, keys, heads):
    return pl.CostEstimate(
        flops=4 * tokens * keys * heads * HD,
        bytes_accessed=8 * tokens * heads * HD,
        transcendentals=tokens * keys * heads,
    )


IN_VMEM = pl.BlockSpec(memory_space=pltpu.VMEM)
IN_SMEM = pl.BlockSpec(memory_space=pltpu.SMEM)
ANYWHERE = pl.BlockSpec(memory_space=pl.ANY)


def later_sums(listed, query, query_first, keys, values, first, heads, others):
    tokens = query.shape[0]
    return pl.pallas_call(
        functools.partial(later_kernel, query_first, first, heads),
        in_specs=[IN_SMEM] + [IN_VMEM] * (3 + len(others)),
        out_specs=IN_VMEM,
        out_shape=jax.ShapeDtypeStruct((heads * HD + stat_rows(heads), tokens), jnp.bfloat16),
        scratch_shapes=[
            pltpu.VMEM((listed.shape[0], 2, tokens, heads * HD), jnp.bfloat16),
        ],
        cost_estimate=estimate(tokens, 5 * tokens, heads),
        compiler_params=pltpu.CompilerParams(vmem_limit_bytes=VMEM_LIMIT),
        name="later",
    )(listed, query, keys, values, *others)


def own_attention(listed, reach, query, keys, values, first, heads, halos, others, returned, out, shape):
    tokens, channels = query.shape
    early = returned is None
    operands = [listed, reach, query, keys, values, *halos, *others]
    if not early:
        operands.append(returned)
    specs = [IN_SMEM] * 2 + [IN_VMEM] * (len(operands) - 2)
    kernel = functools.partial(own_kernel, first, heads, shape, len(halos), early)
    if not early:
        return with_output(kernel, operands, specs, heads, tokens, channels, out, 5 * tokens)
    return pl.pallas_call(
        kernel,
        in_specs=specs,
        out_specs=[IN_VMEM] * 2,
        out_shape=[
            jax.ShapeDtypeStruct((heads * HD, tokens), jnp.float32),
            jax.ShapeDtypeStruct((-(-2 * heads // 8) * 8, tokens), jnp.float32),
        ],
        cost_estimate=estimate(tokens, 5 * tokens, heads),
        compiler_params=pltpu.CompilerParams(vmem_limit_bytes=VMEM_LIMIT),
        name="early",
    )(*operands)


def merged(listed, sums, stats, returned, first, heads, out, tokens, channels):
    operands = [listed, sums, stats, returned]
    kernel = functools.partial(merge_kernel, first, heads)
    specs = [IN_SMEM] + [IN_VMEM] * 3
    return with_output(kernel, operands, specs, heads, tokens, channels, out, tokens)


def with_output(kernel, operands, specs, heads, tokens, channels, out, keys):
    aliases = {}
    if out is not None:
        aliases = {len(operands): 0}
        operands = [*operands, out]
        specs = [*specs, ANYWHERE]
    return pl.pallas_call(
        kernel,
        in_specs=specs,
        out_specs=ANYWHERE,
        out_shape=jax.ShapeDtypeStruct((tokens, channels), jnp.bfloat16),
        scratch_shapes=[
            pltpu.VMEM((heads, tokens, HD), jnp.bfloat16),
            pltpu.SemaphoreType.DMA((heads,)),
        ],
        input_output_aliases=aliases,
        cost_estimate=estimate(tokens, keys, heads),
        compiler_params=pltpu.CompilerParams(vmem_limit_bytes=VMEM_LIMIT),
        name="own",
    )(*operands)


def local(queries, keys, values, neighbours, halo_rows):
    frames, tile_rows, grid_columns, channels = queries.shape
    tokens = frames * tile_rows * grid_columns
    blocks, tiles = lax.axis_size("tm"), lax.axis_size("tile")
    assert blocks % LEVEL == 0 and HMAX <= tile_rows

    def shifted(value, axis, steps):
        size = lax.axis_size(axis)
        return lax.ppermute(
            value, axis, [(i, i + steps) for i in range(size) if 0 <= i + steps < size]
        )

    def swapped(value, bit):
        return lax.ppermute(value, "tm", [(i, i ^ bit) for i in range(blocks)])

    query = queries.reshape(tokens, channels)
    key = keys.reshape(tokens, channels)
    value = values.reshape(tokens, channels)
    listed = neighbours.reshape(-1)
    reach = halo_rows.reshape(-1)
    bounds, first = [], 0
    for heads in CHUNKS:
        bounds.append((first, heads))
        first += heads
    assert first * HD == channels

    across, halos, pairs = [], [], []
    for a, n in bounds:
        lanes = slice(a * HD, (a + n) * HD)
        pair = jnp.concatenate((key[:, lanes], value[:, lanes]), axis=0)
        pair = pair.reshape(2, tokens, n * HD)
        pairs.append(pair)
        across.append(swapped(pair, 2))
        if tiles == 2:
            halos.append([lax.ppermute(pair, "tile", [(0, 1), (1, 0)])])
        else:
            halos.append([shifted(pair, "tile", 1), shifted(pair, "tile", -1)])
    split = CHUNKS[0] * HD
    next_first = shifted(query[:, :split], "tm", -LEVEL)
    next_rest = shifted(query[:, split:], "tm", -LEVEL)
    next_listed = shifted(listed, "tm", -LEVEL)
    beside, corner, below, returned = [], [], [], []
    for pair in pairs:
        beside.append(swapped(pair, 1))
    for at, (first, heads) in enumerate(bounds):
        corner.append(swapped(across[at], 1))
        if at in DIRECT:
            routes = [(i - 1, i) for i in range(LEVEL, blocks, LEVEL)]
            below.append(lax.ppermute(pairs[at], "tm", routes))
        else:
            routes = [(i - LEVEL + 1, i) for i in range(LEVEL, blocks, LEVEL)]
            below.append(lax.ppermute(across[at], "tm", routes))
        sums = later_sums(
            next_listed,
            next_rest if at else next_first,
            first - CHUNKS[0] if at else 0,
            key,
            value,
            first,
            heads,
            [beside[at], across[at], corner[at], below[at]],
        )
        returned.append(shifted(sums, "tm", LEVEL))
    out = None
    for at, (first, heads) in enumerate(bounds):
        early = at in EARLY
        made = own_attention(
            listed,
            reach,
            query,
            key,
            value,
            first,
            heads,
            halos[at],
            [beside[at], across[at], corner[at]],
            None if early else returned[at],
            out,
            (frames, tile_rows, grid_columns),
        )
        if early:
            out = merged(
                listed, *made, returned[at], first, heads, out, tokens, channels
            )
        else:
            out = made
    return out.reshape(frames, tile_rows, grid_columns, channels)


def solution(mesh):
    return jax.shard_map(
        local,
        mesh=mesh,
        in_specs=(
            P("tm", "tile", None, None),
            P("tm", "tile", None, None),
            P("tm", "tile", None, None),
            P("tm", "tile", None),
            P("tm", "tile"),
        ),
        out_specs=P("tm", "tile", None, None),
        check_vma=False,
    )
```
